32 devices in a mesh: vocab: 8 (over z, y), docs: 4 (over x, core).
Axes of the slice: x: 2, y: 2, z: 4, core: 2. Of those that a mesh axis runs over, the one named last changes fastest.
Arguments:
- images: bfloat16 [32768, 4096], P(('vocab', 'docs')), may hold values from -1000 to 1000
- sketch: bfloat16 [4096, 512], replicated, may hold values from -0.09375 to 0.09375
- tile_vals: bfloat16 [32, 32, 2, 64, 128], P(('vocab', 'docs')), as said below
- tile_rows: int32 [32, 32, 2, 64], P(('vocab', 'docs')), may hold values from 0 to 1023
- tile_count: int32 [32, 32], P(('vocab', 'docs')), may hold values from 1 to 2, as said below
- tile_block: int32 [32, 32, 2], P(('vocab', 'docs')), may hold values from 0 to 15
Outputs:
- basis: float32 [65536, 512], P(('vocab', 'docs'))
- factor: float32 [512, 512], replicated
The draws below stay inside these ranges and needn't reach their ends.
Inputs may be any that keep to these rules, and one draw needn't show every extreme that they name: Slots at index tile_count or above hold values that belong to no tile. In every draw some owners receive 2 live slots from every device. `tile_vals`: nonnegative term weights.
All inputs are finite; a program needn't handle non-finite values.
Results may differ from the reference program's by a relative error of at most 0.003.
The reference program's roundings to bfloat16 on the way (of `sketch_scaled` and `projected`) count: a program that leaves them out, or rounds other values in their place, can miss the bound.
Values may be sent and summed in bfloat16 or wider, within the bound.
No kernel may reach another device: no remote copies, remote signals or barrier semaphores. Data moves between devices by JAX's collectives and lax.ppermute only.
A program may use at most 192 MiB of HBM per device.

```python
import math
import jax
import jax.numpy as jnp
from jax import lax

F = 4096
K = 512
TILE = 128
VOCAB_DEV = 2048
TR = 64
CAP = 2
DOC_DEV = 1024
SENDERS = 32
DOCS = 32768


def draw_images(key, part):
    key_cols, key_base = jax.random.split(key, 2)
    devices_count = DOCS // DOC_DEV
    device_of_row = (jnp.arange(DOCS, dtype=jnp.int32) // DOC_DEV).astype(jnp.float32)
    rising = 1.0 + 2.0 * device_of_row / max(devices_count - 1, 1)
    column_scale = jnp.exp(jax.random.uniform(key_cols, (F,), jnp.float32, 0.0, math.log(10.0)))
    values = jnp.clip(jax.random.normal(key_base, (DOCS, F), jnp.float32), -4.0, 4.0)
    return (values * column_scale[None, :] * rising[:, None]).astype(jnp.bfloat16)


def draw_tile_vals(key, part):
    key_keep, key_cols, key_mag = jax.random.split(key, 3)
    shape = (SENDERS, SENDERS, CAP, TR, TILE)
    keeping = jax.random.bernoulli(key_keep, 0.6, shape).astype(jnp.float32)
    column_scale = jnp.exp(jax.random.uniform(key_cols, (SENDERS, SENDERS, CAP, 1, TILE), jnp.float32, 0.0, math.log(10.0)))
    owner_pos = jnp.arange(SENDERS, dtype=jnp.int32).astype(jnp.float32) / max(SENDERS - 1, 1)
    per_column = SENDERS * CAP * TILE * TR / VOCAB_DEV
    base = 1.0 / math.sqrt(8.0 * per_column)
    magnitude = jnp.abs(jnp.clip(jax.random.normal(key_mag, shape, jnp.float32), -4.0, 4.0))
    rising = 1.0 + 2.0 * owner_pos
    values = keeping * magnitude * column_scale * rising[None, :, None, None, None] * base
    return values.astype(jnp.bfloat16)


def draw_tile_count(key, part):
    key_order, key_light = jax.random.split(key, 2)
    ordering = jax.random.permutation(key_order, SENDERS)
    heavy = ordering < max(SENDERS // 8, 1)
    light = jax.random.randint(key_light, (SENDERS, SENDERS), 1, CAP + 1, dtype=jnp.int32)
    return jnp.where(heavy[None, :], CAP, light).astype(jnp.int32)


def set_ends(entries, key, least, top_value):
    place = [jax.random.randint(jax.random.fold_in(key, axis), (), 0, length) for axis, length in enumerate(entries.shape)]
    longest = entries.shape.index(max(entries.shape))
    beside = place[:longest] + [(place[longest] + 1) % entries.shape[longest]] + place[longest + 1:]
    return entries.at[tuple(place)].set(least).at[tuple(beside)].set(top_value)


def centred(rng, dims, width, most, held_as=jnp.bfloat16):
    result = jax.random.normal(rng, dims, jnp.float32) * width
    return jnp.minimum(jnp.maximum(result, -most), most).astype(held_as)


def setup_inputs(seed: int = 0) -> dict:
    key_list = jax.random.split(jax.random.key(seed), 7)
    return {
        "images": draw_images(jax.random.fold_in(key_list[6], 71), 0),
        "sketch": centred(key_list[1], (F, K), F ** -0.5, 0.09375),
        "tile_vals": draw_tile_vals(jax.random.fold_in(key_list[6], 71), 0),
        "tile_rows": set_ends(jax.random.randint(key_list[3], (SENDERS, SENDERS, CAP, TR), 0, DOC_DEV), jax.random.fold_in(key_list[3], 1), 0, DOC_DEV - 1).astype(jnp.int32),
        "tile_count": draw_tile_count(jax.random.fold_in(key_list[6], 71), 0),
        "tile_block": set_ends(jax.random.randint(key_list[5], (SENDERS, SENDERS, CAP), 0, VOCAB_DEV // TILE), jax.random.fold_in(key_list[5], 1), 0, (VOCAB_DEV // TILE) - 1).astype(jnp.int32),
    }


def reference(images, sketch, tile_vals, tile_rows, tile_count, tile_block):
    senders = tile_count.shape[0]
    doc_total = images.shape[0]
    power = lax.optimization_barrier(jnp.sum(jnp.square(images.astype(jnp.float32)), axis=0))
    scales = lax.rsqrt(power / doc_total + 1e-05)
    sketch_scaled = (sketch.astype(jnp.float32) * scales[:, None]).astype(jnp.bfloat16)
    projected = jnp.dot(images.astype(jnp.float32), sketch_scaled.astype(jnp.float32), preferred_element_type=jnp.float32).astype(jnp.bfloat16)
    block_count = VOCAB_DEV // TILE
    slot_index = lax.broadcasted_iota(jnp.int32, (senders, CAP), 1)
    offsets = (jnp.arange(senders, dtype=jnp.int32) * DOC_DEV)[:, None, None]
    block_iota = jnp.arange(block_count, dtype=jnp.int32)

    def owner(target):
        values = tile_vals[:, target]
        alive_mask = slot_index < tile_count[:, target][:, None]
        values = jnp.where(alive_mask[:, :, None, None], values.astype(jnp.float32), 0.0)
        values = values.reshape(senders * CAP, TR, TILE)
        rows = (tile_rows[:, target] + offsets).astype(jnp.int32)
        picked = projected[rows].astype(jnp.float32).reshape(senders * CAP, TR, K)
        product = jnp.einsum('srk,srj->skj', values, picked, precision=lax.Precision.HIGHEST)
        slot_hot = (tile_block[target].reshape(senders * CAP)[:, None] == block_iota[None, :]).astype(jnp.float32)
        summed = jnp.einsum('sb,skj->bkj', slot_hot, product, precision=lax.Precision.HIGHEST)
        squares = jnp.einsum('sb,sk->bk', slot_hot, lax.optimization_barrier(jnp.sum(values * values, axis=1)), precision=lax.Precision.HIGHEST)
        summed = summed * lax.rsqrt(squares + 1.0)[:, :, None]
        return summed.reshape(VOCAB_DEV, K)
    stacked = lax.map(owner, jnp.arange(senders, dtype=jnp.int32))
    whole = stacked.reshape(senders * VOCAB_DEV, K)
    gram_first = jnp.dot(whole.T, whole, precision=lax.Precision.HIGHEST)
    lower_first = jnp.linalg.cholesky(gram_first)
    basis_first = jax.scipy.linalg.solve_triangular(lower_first, whole.T, lower=True)
    root = jnp.sqrt(jnp.float32(whole.shape[0]))
    factor = lower_first.T / root
    return (basis_first.T * root, factor)
```

```python
import math

import jax
import jax.numpy as jnp
from jax import lax
from jax.experimental import pallas as pl
from jax.experimental.pallas import tpu as pltpu
from jax.sharding import PartitionSpec as P


VOCAB_DEV = 2048
LANES = 128
FIRST_PART = 3
BOTH = ("half", "rest", "docs")
SIDE = ("rest", "docs")
F32 = jnp.float32
BF16 = jnp.bfloat16
FULL_VMEM = pl.BlockSpec(memory_space=pltpu.VMEM)
IN_HBM = pl.BlockSpec(memory_space=pltpu.HBM)
IN_SMEM = pl.BlockSpec(memory_space=pltpu.SMEM)


def cost(micros, moved=0):
    return pl.CostEstimate(flops=int(micros * 1e9), bytes_accessed=moved, transcendentals=0)


def params(mebibytes):
    return pltpu.CompilerParams(vmem_limit_bytes=mebibytes * 1024 * 1024)


def split2(x):
    high = x.astype(BF16)
    return high, (x - high.astype(F32)).astype(BF16)


def split3(x):
    high = x.astype(BF16).astype(F32)
    rest = x - high
    middle = rest.astype(BF16).astype(F32)
    return high, middle, rest - middle


def dot(a, b, ca, cb):
    return lax.dot_general(a, b, (((ca,), (cb,)), ((), ())), preferred_element_type=F32)


def exact(a, b, ca, cb):
    return lax.dot_general(
        a, b, (((ca,), (cb,)), ((), ())), preferred_element_type=F32, precision=lax.Precision.HIGHEST
    )


def prepare_kernel(steps, count_ref, images_hbm, vals_hbm, out_ref, power_ref, images_ref, vals_ref, arrivals):
    docs, features = images_ref.shape
    rows = docs // steps
    copies = [pltpu.make_async_copy(vals_hbm.at[0], vals_ref, arrivals.at[steps])]
    for i in range(steps):
        at = pl.ds(i * rows, rows)
        copies.append(pltpu.make_async_copy(images_hbm.at[at], images_ref.at[at], arrivals.at[i]))
    for copy in copies:
        copy.start()
    copies[0].wait()
    senders, capacity = vals_ref.shape[:2]

    def mask(o, carry):
        live = count_ref[0, o]
        for c in range(capacity):
            out_ref[o, c] = vals_ref[o, c] * jnp.where(c < live, 1.0, 0.0).astype(BF16)
        return carry

    lax.fori_loop(0, senders, mask, 0)
    wide = 1024
    totals = [jnp.zeros((8, wide), F32) for _ in range(features // wide)]
    for i in range(steps):
        copies[1 + i].wait()
        for f in range(features // wide):

            def group(r, total):
                at = pl.multiple_of(i * rows + r * 32, 32)
                values = images_ref[pl.ds(at, 32), f * wide : (f + 1) * wide].astype(F32)
                values = values * values
                return total + ((values[:8] + values[8:16]) + (values[16:24] + values[24:]))

            totals[f] = lax.fori_loop(0, rows // 32, group, totals[f])
    for f in range(features // wide):
        power_ref[:, f * wide : (f + 1) * wide] = jnp.sum(totals[f], axis=0, keepdims=True)


def prepare(count, images, vals):
    docs, features = images.shape
    steps = 8
    return pl.pallas_call(
        lambda *refs: prepare_kernel(steps, *refs),
        in_specs=[IN_SMEM, IN_HBM, IN_HBM],
        out_specs=(FULL_VMEM, FULL_VMEM),
        out_shape=(
            jax.ShapeDtypeStruct(vals.shape[1:], BF16),
            jax.ShapeDtypeStruct((1, features), F32),
        ),
        scratch_shapes=[
            pltpu.VMEM((docs, features), BF16),
            pltpu.VMEM(vals.shape[1:], BF16),
            pltpu.SemaphoreType.DMA((steps + 1,)),
        ],
        compiler_params=params(58),
        cost_estimate=cost(4),
        name="prepare",
    )(count, images, vals)


def project_kernel(
    documents, steps, power_ref, images_hbm, sketch_hbm, first_ref, second_ref, images_ref, sketch_ref, scaled_ref, arrivals
):
    features, columns = sketch_ref.shape
    docs = images_ref.shape[0]
    rows = docs // steps
    deep = features // steps
    copies = []
    for i in range(steps):
        at = pl.ds(i * deep, deep)
        copies.append(pltpu.make_async_copy(sketch_hbm.at[at], sketch_ref.at[at], arrivals.at[i]))
    for i in range(steps):
        at = pl.ds(i * rows, rows)
        copies.append(pltpu.make_async_copy(images_hbm.at[at], images_ref.at[at], arrivals.at[steps + i]))
    for copy in copies:
        copy.start()
    for i in range(steps):
        copies[i].wait()
        for k in range(i * deep, (i + 1) * deep, LANES):
            scale = lax.rsqrt(power_ref[:, k : k + LANES] / documents + 1e-05)
            scale = jnp.broadcast_to(scale, (LANES, LANES)).T
            scale = jnp.concatenate([scale] * (columns // LANES), axis=1)
            scaled_ref[k : k + LANES, :] = (sketch_ref[k : k + LANES, :].astype(F32) * scale).astype(BF16)
    cut = first_ref.shape[1]
    for i in range(steps):
        copies[steps + i].wait()
        at = slice(i * rows, (i + 1) * rows)
        found = jnp.dot(images_ref[at, :], scaled_ref[...], preferred_element_type=F32).astype(BF16)
        first_ref[at, :] = found[:, :cut]
        second_ref[at, :] = found[:, cut:]


def project(power, images, sketch, documents, cut):
    docs = images.shape[0]
    _, columns = sketch.shape
    steps = 4
    return pl.pallas_call(
        lambda *refs: project_kernel(documents, steps, *refs),
        in_specs=[FULL_VMEM, IN_HBM, IN_HBM],
        out_specs=(FULL_VMEM, FULL_VMEM),
        out_shape=(
            jax.ShapeDtypeStruct((docs, cut), BF16),
            jax.ShapeDtypeStruct((docs, columns - cut), BF16),
        ),
        scratch_shapes=[
            pltpu.VMEM(images.shape, BF16),
            pltpu.VMEM(sketch.shape, BF16),
            pltpu.VMEM(sketch.shape, BF16),
            pltpu.SemaphoreType.DMA((2 * steps,)),
        ],
        compiler_params=params(58),
        cost_estimate=cost(7),
        name="project",
    )(power, images, sketch)


def gather_kernel(index_ref, table_ref, out_ref):
    docs = table_ref.shape[0]
    group, _, rows = index_ref.shape
    lane = lax.broadcasted_iota(jnp.int32, (rows, LANES), 1).astype(F32)
    hots = []
    for g in range(group):
        index = jnp.broadcast_to(index_ref[g].astype(F32), (LANES, rows)).T
        hots.append(
            jnp.concatenate(
                [jnp.where(index == lane + float(k), 1.0, 0.0).astype(BF16) for k in range(0, docs, LANES)],
                axis=1,
            )
        )
    found = jnp.dot(jnp.concatenate(hots, axis=0), table_ref[...], preferred_element_type=F32)
    out_ref[...] = found.astype(BF16).reshape(out_ref.shape)


def gather_rows(index, table):
    senders, rows = index.shape
    docs, columns = table.shape
    group = 4
    return pl.pallas_call(
        gather_kernel,
        grid=(senders // group,),
        in_specs=[
            pl.BlockSpec((group, 1, rows), lambda s: (s, 0, 0)),
            pl.BlockSpec((docs, columns), lambda s: (0, 0)),
        ],
        out_specs=pl.BlockSpec((group, rows, columns), lambda s: (s, 0, 0)),
        out_shape=jax.ShapeDtypeStruct((senders, rows, columns), BF16),
        compiler_params=params(58),
        cost_estimate=cost(3),
        name="gather_rows",
    )(index.reshape(senders, 1, rows), table)


def scale_kernel(block_ref, vals_ref, scale_ref, turned_ref, square_ref):
    square_ref[...] = jnp.zeros_like(square_ref)

    def slot(s, carry):
        weights = vals_ref[s].astype(F32)
        block = block_ref[s]
        square_ref[pl.ds(block, 1), :] += jnp.sum(weights * weights, axis=0, keepdims=True)
        turned_ref[s] = vals_ref[s].T
        return carry

    lax.fori_loop(0, vals_ref.shape[0], slot, 0)
    width = vals_ref.shape[2]
    for b in range(square_ref.shape[0]):
        root = lax.rsqrt(square_ref[b : b + 1, :] + 1.0)
        scale_ref[b * width : (b + 1) * width, :] = jnp.broadcast_to(root, (LANES, width)).T


def row_scales(blocks, vals):
    width = vals.shape[2]
    count = VOCAB_DEV // width
    return pl.pallas_call(
        scale_kernel,
        in_specs=[IN_SMEM, FULL_VMEM],
        out_specs=(FULL_VMEM, FULL_VMEM),
        out_shape=(
            jax.ShapeDtypeStruct((VOCAB_DEV, LANES), F32),
            jax.ShapeDtypeStruct((vals.shape[0], width, vals.shape[1]), BF16),
        ),
        scratch_shapes=[pltpu.VMEM((count, width), F32)],
        compiler_params=params(58),
        cost_estimate=cost(3),
        name="row_scales",
    )(blocks, vals)


def collect_kernel(earlier, sources, half_ref, block_ref, vals_hbm, scale_hbm, *refs):
    count = 2 * earlier
    rows_hbm, refs = refs[:sources], refs[sources:]
    before_hbm = refs[:count]
    high_ref, low_ref, gram_ref, sum_ref, vals_ref, scale_ref = refs[count : count + 6]
    rows_refs, refs = refs[count + 6 : count + 6 + sources], refs[count + 6 + sources :]
    before, arrivals = refs[:count], refs[count]
    slots, width, _ = vals_ref.shape
    columns = high_ref.shape[1]
    part = slots // sources
    half = half_ref[0]
    starts = [0] if sources == 1 else [half * part, (1 - half) * part]
    moves = []
    for i in range(sources):
        moves.append((vals_hbm.at[pl.ds(starts[i], part)], vals_ref.at[pl.ds(i * part, part)]))
        moves.append((rows_hbm[i], rows_refs[i]))
    moves.append((scale_hbm, scale_ref))
    moves += list(zip(before_hbm, before))
    copies = [pltpu.make_async_copy(src, dst, arrivals.at[i]) for i, (src, dst) in enumerate(moves)]
    for copy in copies:
        copy.start()
    sum_ref[...] = jnp.zeros_like(sum_ref)
    unroll = 8

    for i in range(sources):
        copies[2 * i].wait()
        copies[2 * i + 1].wait()

        def group(g, carry):
            parts = [
                jnp.dot(
                    vals_ref[i * part + g * unroll + u],
                    rows_refs[i][g * unroll + u],
                    preferred_element_type=F32,
                )
                for u in range(unroll)
            ]
            for u in range(unroll):
                at = pl.multiple_of(block_ref[starts[i] + g * unroll + u] * width, width)
                sum_ref[pl.ds(at, width), :] += parts[u]
            return carry

        lax.fori_loop(0, part // unroll, group, 0)
    for copy in copies[2 * sources :]:
        copy.wait()
    gram_ref[...] = jnp.zeros_like(gram_ref)
    step = 512

    def tile(t, carry):
        at = pl.ds(pl.multiple_of(t * step, step), step)
        scale = scale_ref[at, :]
        whole = sum_ref[at, :] * jnp.concatenate([scale] * (columns // LANES), axis=1)
        high, low = split2(whole)
        high_ref[at, :] = high
        low_ref[at, :] = low
        place = 0
        for e in range(earlier + 1):
            if e < earlier:
                other_high, other_low = before[2 * e][at, :], before[2 * e + 1][at, :]
            else:
                other_high, other_low = high, low
            wide = other_high.shape[1]
            gram_ref[:, place : place + wide] += (
                dot(high, other_high, 0, 0) + dot(low, other_high, 0, 0) + dot(high, other_low, 0, 0)
            )
            place += wide
        return carry

    lax.fori_loop(0, VOCAB_DEV // step, tile, 0)


def collect(half, blocks, vals, scales, rows, before):
    columns = rows[0].shape[2]
    known = sum(high.shape[1] for high, low in before)
    flat = [piece for pair in before for piece in pair]
    moved = len(rows) * 2 + 1 + len(flat)
    return pl.pallas_call(
        lambda *refs: collect_kernel(len(before), len(rows), *refs),
        in_specs=[IN_SMEM] * 2 + [IN_HBM] * (2 + len(rows) + len(flat)),
        out_specs=(FULL_VMEM,) * 3,
        out_shape=(
            jax.ShapeDtypeStruct((VOCAB_DEV, columns), BF16),
            jax.ShapeDtypeStruct((VOCAB_DEV, columns), BF16),
            jax.ShapeDtypeStruct((columns, known + columns), F32),
        ),
        scratch_shapes=[
            pltpu.VMEM((VOCAB_DEV, columns), F32),
            pltpu.VMEM(vals.shape, BF16),
            pltpu.VMEM(scales.shape, F32),
        ]
        + [pltpu.VMEM(piece.shape, BF16) for piece in list(rows) + flat]
        + [pltpu.SemaphoreType.DMA((moved,))],
        compiler_params=params(58),
        cost_estimate=cost(5),
        name="collect",
    )(half, blocks, vals, scales, *rows, *flat)


def factor_block(rest_ref, unit_ref, upper_ref, inverse_ref):
    size = rest_ref.shape[0]
    lane = lax.broadcasted_iota(jnp.int32, (8, size), 1)
    sub = lax.broadcasted_iota(jnp.int32, (8, size), 0)

    def spread(row):
        return jnp.broadcast_to(row, (8, size))

    def panel(p, carry):
        first = pl.multiple_of(p * 8, 8)
        rows = rest_ref[pl.ds(first, 8), :]
        inverse = unit_ref[pl.ds(first, 8), :]
        columns = [
            spread(jnp.sum(jnp.where(lane == first + j, rows, 0.0), axis=1, keepdims=True))
            for j in range(8)
        ]
        for j in range(8):
            root = lax.rsqrt(spread(columns[j][j : j + 1, :]))
            lower = columns[j] * root
            for m in range(j + 1, 8):
                columns[m] = columns[m] - lower * spread(lower[m : m + 1, :])
            below = jnp.where(sub > j, lower, 0.0)
            row = spread(rows[j : j + 1, :]) * root
            rows = jnp.where(sub == j, row, rows - below * row)
            row = spread(inverse[j : j + 1, :]) * root
            inverse = jnp.where(sub == j, row, inverse - below * row)
        rows = jnp.where(lane >= first + sub, rows, 0.0)
        upper_ref[pl.ds(first, 8), :] = rows
        inverse_ref[pl.ds(first, 8), :] = inverse
        a, b, c = split3(rows)
        x, y, z = split3(inverse)
        left = jnp.concatenate([a, a, b, a, c, b], axis=0).T.astype(BF16)
        right = jnp.concatenate(
            [jnp.concatenate([a, b, a, c, a, b], axis=0), jnp.concatenate([x, y, x, z, x, y], axis=0)],
            axis=1,
        ).astype(BF16)
        update = jnp.dot(left, right, preferred_element_type=F32)
        rest_ref[...] -= update[:, :size]
        unit_ref[...] -= update[:, size:]
        return carry

    lax.fori_loop(0, size // 8, panel, 0)


def cholesky_kernel(row, root, last, count, gram_ref, *refs):
    refs = list(refs)
    size = LANES
    if count:
        known_ref = refs.pop(0)
    before = [refs.pop(0) for _ in range(count if last else 0)]
    inverse_ref, upper_ref, rest_ref, unit_ref, piece_ref, small_ref = refs
    known = count * size
    mine = slice(row * size, (row + 1) * size)
    corner = gram_ref[mine, known : known + size]
    if count:
        left = exact(gram_ref[mine, :known], known_ref[...], 1, 1)
        corner = corner - exact(left, left, 1, 1)
    rest_ref[...] = corner
    square = (size, size)
    unit_ref[...] = jnp.where(
        lax.broadcasted_iota(jnp.int32, square, 0) == lax.broadcasted_iota(jnp.int32, square, 1), 1.0, 0.0
    )
    factor_block(rest_ref, unit_ref, piece_ref, small_ref)
    small = small_ref[...]
    place = known if last else 0
    if last:
        upper_ref[...] = jnp.zeros_like(upper_ref)
        for e in range(count):
            upper_ref[: (e + 1) * size, e * size : (e + 1) * size] = before[e][...]
    if count:
        inverse_ref[:known, :known] = known_ref[...]
        inverse_ref[:known, known:] = jnp.zeros((known, size), F32)
        inverse_ref[known:, :known] = -exact(small, exact(left, known_ref[...], 1, 0), 1, 0)
        upper_ref[:known, place : place + size] = left.T * (1.0 / root)
    inverse_ref[known:, known:] = small
    upper_ref[known:, place : place + size] = piece_ref[...] * (1.0 / root)


def cholesky_step(gram, row, inverse, before, root, last):
    count = len(before)
    total = (count + 1) * LANES
    inputs = [gram] + ([inverse] if count else []) + (list(before) if last else [])
    square = pltpu.VMEM((LANES, LANES), F32)
    return pl.pallas_call(
        lambda *refs: cholesky_kernel(row, root, last, count, *refs),
        in_specs=[FULL_VMEM] * len(inputs),
        out_specs=(FULL_VMEM,) * 2,
        out_shape=(
            jax.ShapeDtypeStruct((total, total), F32),
            jax.ShapeDtypeStruct((total, total if last else LANES), F32),
        ),
        scratch_shapes=[square] * 4,
        compiler_params=params(16),
        cost_estimate=cost(8),
        name="cholesky_step",
    )(*inputs)


def basis_kernel(pieces, known, root, inverse_ref, *refs):
    out_ref = refs[-1]
    total = None
    place = 0
    for e in range(pieces):
        high, low = refs[2 * e][...], refs[2 * e + 1][...]
        wide = high.shape[1]
        part_high, part_low = split2(inverse_ref[known:, place : place + wide])
        term = dot(high, part_high, 1, 1) + dot(low, part_high, 1, 1) + dot(high, part_low, 1, 1)
        total = term if total is None else total + term
        place += wide
    out_ref[...] = total * root


def basis_block(inverse, pieces, buffer, root, columns_total):
    columns = pieces[-1][0].shape[1]
    total = inverse.shape[0]
    known = total - columns
    step = 512
    flat = [piece for pair in pieces for piece in pair]
    in_specs = [pl.BlockSpec((total, total), lambda t: (0, 0))]
    in_specs += [pl.BlockSpec((step, piece.shape[1]), lambda t: (t, 0)) for piece in flat]
    inputs = [inverse] + flat
    aliases = {}
    if buffer is not None:
        aliases = {len(inputs): 0}
        inputs.append(buffer)
        in_specs.append(pl.BlockSpec(memory_space=pl.ANY))
    return pl.pallas_call(
        lambda *refs: basis_kernel(len(pieces), known, root, *refs),
        grid=(VOCAB_DEV // step,),
        in_specs=in_specs,
        out_specs=pl.BlockSpec((step, columns), lambda t: (t, known // columns)),
        out_shape=jax.ShapeDtypeStruct((VOCAB_DEV, columns_total), F32),
        input_output_aliases=aliases,
        compiler_params=params(58),
        cost_estimate=cost(3),
        name="basis_block",
    )(*inputs)


def swap(x, axis, bit):
    size = lax.axis_size(axis)
    return lax.ppermute(x, axis, [(i, i ^ bit) for i in range(size)])


def bits(axis):
    size = lax.axis_size(axis)
    return [1 << k for k in range(size.bit_length() - 1)]


def sum_all(x):
    for axis in ("docs", "rest", "half"):
        for bit in bits(axis):
            x = x + swap(x, axis, bit)
    return x


def sum_halves(x):
    half = x.shape[0] // 2
    odd = lax.axis_index("docs") % 2
    mine = lax.dynamic_slice_in_dim(x, odd * half, half)
    other = lax.dynamic_slice_in_dim(x, (1 - odd) * half, half)
    mine = mine + swap(other, "docs", 1)
    for axis in ("docs", "rest", "half"):
        for bit in bits(axis):
            if axis != "docs" or bit > 1:
                mine = mine + swap(mine, axis, bit)
    other = swap(mine, "docs", 1)
    return jnp.concatenate(
        [jnp.where(odd == 0, mine, other), jnp.where(odd == 0, other, mine)], axis=0
    )


def body(images, sketch, tile_vals, tile_rows, tile_count, tile_block):
    side = lax.axis_size("rest") * lax.axis_size("docs")
    senders = 2 * side
    doc_rows = images.shape[0]
    capacity, tile_height, tile_width = tile_vals.shape[2:]
    columns = sketch.shape[1]
    slots = senders * capacity
    cut = FIRST_PART * LANES
    half = lax.axis_index("half")
    outgoing, power = prepare(tile_count, images, tile_vals)
    vals = lax.all_to_all(
        outgoing.reshape(senders, capacity * tile_height, tile_width), BOTH, 0, 0, tiled=True
    )
    vals = vals.reshape(slots, tile_height, tile_width)
    power = sum_all(power)
    index = tile_rows[0].reshape(senders, capacity * tile_height)
    halves = index.reshape(2, side, capacity * tile_height)
    near_index = lax.dynamic_index_in_dim(halves, half, 0, keepdims=False)
    far_index = swap(lax.dynamic_index_in_dim(halves, 1 - half, 0, keepdims=False), "half", 1)
    blocks = tile_block[0].reshape(slots)
    root = math.sqrt(VOCAB_DEV * senders)
    scale, turned = row_scales(blocks, vals)
    where = half.reshape(1).astype(jnp.int32)
    table, last_table = project(power, images, sketch, doc_rows * senders, cut)
    far_table = swap(table, "half", 1)
    near = gather_rows(near_index, table)
    near = lax.all_to_all(near, SIDE, 0, 0, tiled=True)
    far = gather_rows(far_index, far_table)
    far = lax.all_to_all(far, SIDE, 0, 0, tiled=True)
    final = gather_rows(index, last_table)
    final = lax.all_to_all(final, BOTH, 0, 0, tiled=True)

    def by_slot(rows):
        return rows.reshape(-1, tile_height, rows.shape[2])

    pieces, uppers = [], []
    inverse = basis = None
    for rows in [[by_slot(near), by_slot(far)], [by_slot(final)]]:
        high, low, gram = collect(where, blocks, turned, scale, rows, pieces)
        pieces.append((high, low))
        gram = sum_halves(gram)
        for row in range(gram.shape[0] // LANES):
            last = (len(uppers) + 1) * LANES == columns
            inverse, upper = cholesky_step(gram, row, inverse, uppers, root, last)
            uppers.append(upper)
        basis = basis_block(inverse, pieces, basis, root, columns)
    return (basis, uppers[-1])


def solution(mesh):
    split = (2, mesh.shape["vocab"] // 2, mesh.shape["docs"])
    finer = jax.sharding.Mesh(mesh.devices.reshape(split), BOTH)
    placed = (
        P(BOTH, None),
        P(),
        P(BOTH, None, None, None, None),
        P(BOTH, None, None, None),
        P(BOTH, None),
        P(BOTH, None, None),
    )
    return jax.shard_map(
        body,
        mesh=finer,
        in_specs=placed,
        out_specs=(P(BOTH, None), P()),
        check_vma=False,
    )
```

```python
import math

import jax
import jax.numpy as jnp
from jax import lax
from jax.experimental import pallas as pl
from jax.experimental.pallas import tpu as pltpu
from jax.sharding import PartitionSpec as P


VOCAB_DEV = 2048
LANES = 128
FIRST_PART = 3
BOTH = ("half", "rest", "docs")
SIDE = ("rest", "docs")
F32 = jnp.float32
BF16 = jnp.bfloat16
FULL_VMEM = pl.BlockSpec(memory_space=pltpu.VMEM)
IN_HBM = pl.BlockSpec(memory_space=pltpu.HBM)
IN_SMEM = pl.BlockSpec(memory_space=pltpu.SMEM)


def cost(micros, moved=0):
    return pl.CostEstimate(flops=int(micros * 1e9), bytes_accessed=moved, transcendentals=0)


def params(mebibytes):
    return pltpu.CompilerParams(vmem_limit_bytes=mebibytes * 1024 * 1024)


def split2(x):
    high = x.astype(BF16)
    return high, (x - high.astype(F32)).astype(BF16)


def split3(x):
    high = x.astype(BF16).astype(F32)
    rest = x - high
    middle = rest.astype(BF16).astype(F32)
    return high, middle, rest - middle


def dot(a, b, ca, cb):
    return lax.dot_general(a, b, (((ca,), (cb,)), ((), ())), preferred_element_type=F32)


def exact(a, b, ca, cb):
    return lax.dot_general(
        a, b, (((ca,), (cb,)), ((), ())), preferred_element_type=F32, precision=lax.Precision.HIGHEST
    )


def prepare_kernel(steps, count_ref, images_hbm, vals_hbm, out_ref, power_ref, images_ref, vals_ref, arrivals):
    docs, features = images_ref.shape
    rows = docs // steps
    copies = [pltpu.make_async_copy(vals_hbm.at[0], vals_ref, arrivals.at[steps])]
    for i in range(steps):
        at = pl.ds(i * rows, rows)
        copies.append(pltpu.make_async_copy(images_hbm.at[at], images_ref.at[at], arrivals.at[i]))
    for copy in copies:
        copy.start()
    copies[0].wait()
    senders, capacity = vals_ref.shape[:2]

    def mask(o, carry):
        live = count_ref[0, o]
        for c in range(capacity):
            out_ref[o, c] = vals_ref[o, c] * jnp.where(c < live, 1.0, 0.0).astype(BF16)
        return carry

    lax.fori_loop(0, senders, mask, 0)
    wide = 1024
    totals = [jnp.zeros((8, wide), F32) for _ in range(features // wide)]
    for i in range(steps):
        copies[1 + i].wait()
        for f in range(features // wide):

            def group(r, total):
                at = pl.multiple_of(i * rows + r * 32, 32)
                values = images_ref[pl.ds(at, 32), f * wide : (f + 1) * wide].astype(F32)
                values = values * values
                return total + ((values[:8] + values[8:16]) + (values[16:24] + values[24:]))

            totals[f] = lax.fori_loop(0, rows // 32, group, totals[f])
    for f in range(features // wide):
        power_ref[:, f * wide : (f + 1) * wide] = jnp.sum(totals[f], axis=0, keepdims=True)


def prepare(count, images, vals):
    docs, features = images.shape
    steps = 8
    return pl.pallas_call(
        lambda *refs: prepare_kernel(steps, *refs),
        in_specs=[IN_SMEM, IN_HBM, IN_HBM],
        out_specs=(FULL_VMEM, FULL_VMEM),
        out_shape=(
            jax.ShapeDtypeStruct(vals.shape[1:], BF16),
            jax.ShapeDtypeStruct((1, features), F32),
        ),
        scratch_shapes=[
            pltpu.VMEM((docs, features), BF16),
            pltpu.VMEM(vals.shape[1:], BF16),
            pltpu.SemaphoreType.DMA((steps + 1,)),
        ],
        compiler_params=params(58),
        cost_estimate=cost(4),
        name="prepare",
    )(count, images, vals)


def hot_rows(index, docs):
    rows = index.shape[1]
    spread = jnp.broadcast_to(index.astype(F32), (LANES, rows)).T
    lane = lax.broadcasted_iota(jnp.int32, (rows, LANES), 1).astype(F32)
    return jnp.concatenate(
        [jnp.where(spread == lane + float(k), 1.0, 0.0).astype(BF16) for k in range(0, docs, LANES)], axis=1
    )


def project_kernel(documents, steps, group, power_ref, index_ref, images_hbm, sketch_hbm, *refs):
    outputs = refs[:3]
    images_ref, sketch_ref, scaled_ref, sum_ref, hot_ref, first_ref, second_ref, near_ref = refs[3:11]
    arrivals, departures = refs[11:]
    docs = images_ref.shape[1]
    features, columns = sketch_ref.shape
    deep = features // steps
    copies = []
    for i in range(steps):
        at = pl.ds(i * deep, deep)
        copies.append(pltpu.make_async_copy(sketch_hbm.at[at], sketch_ref.at[at], arrivals.at[i]))
        copies.append(pltpu.make_async_copy(images_hbm.at[:, at], images_ref.at[i], arrivals.at[steps + i]))
    for copy in copies:
        copy.start()
    owners, _, rows = index_ref.shape

    def build(o, carry):
        hot_ref[pl.ds(pl.multiple_of(o * rows, rows), rows), :] = hot_rows(index_ref[o], docs)
        return carry

    lax.fori_loop(0, owners, build, 0)
    cut = first_ref.shape[1]
    for i in range(steps):
        copies[2 * i].wait()
        for k in range(i * deep, (i + 1) * deep, LANES):
            scale = lax.rsqrt(power_ref[:, k : k + LANES] / documents + 1e-05)
            scale = jnp.broadcast_to(scale, (LANES, LANES)).T
            scale = jnp.concatenate([scale] * (columns // LANES), axis=1)
            scaled_ref[k : k + LANES, :] = (sketch_ref[k : k + LANES, :].astype(F32) * scale).astype(BF16)
        copies[2 * i + 1].wait()
        for r in range(0, docs, docs // 2):
            at = slice(r, r + docs // 2)
            part = jnp.dot(
                images_ref[i, at, :], scaled_ref[i * deep : (i + 1) * deep, :], preferred_element_type=F32
            )
            if i:
                part = sum_ref[at, :] + part
            if i < steps - 1:
                sum_ref[at, :] = part
            else:
                found = part.astype(BF16)
                first_ref[at, :] = found[:, :cut]
                second_ref[at, :] = found[:, cut:]
    sent = [
        pltpu.make_async_copy(first_ref, outputs[0], departures.at[0]),
        pltpu.make_async_copy(second_ref, outputs[1], departures.at[1]),
    ]
    for copy in sent:
        copy.start()
    for g in range(owners // group):
        hot = hot_ref[g * group * rows : (g + 1) * group * rows, :]
        found = jnp.dot(hot, first_ref[...], preferred_element_type=F32).astype(BF16)
        at = slice(g * group, (g + 1) * group)
        near_ref[at] = found.reshape(group, rows, cut)
        copy = pltpu.make_async_copy(
            near_ref.at[pl.ds(g * group, group)], outputs[2].at[pl.ds(g * group, group)], departures.at[2 + g]
        )
        copy.start()
        sent.append(copy)
    for copy in sent:
        copy.wait()


def project(power, index, images, sketch, documents, cut):
    docs, features = images.shape
    columns = sketch.shape[1]
    owners, rows = index.shape
    steps, group = 4, 4
    shapes = [
        jax.ShapeDtypeStruct((docs, cut), BF16),
        jax.ShapeDtypeStruct((docs, columns - cut), BF16),
        jax.ShapeDtypeStruct((owners, rows, cut), BF16),
    ]
    return pl.pallas_call(
        lambda *refs: project_kernel(documents, steps, group, *refs),
        in_specs=[FULL_VMEM, FULL_VMEM, IN_HBM, IN_HBM],
        out_specs=(IN_HBM,) * 3,
        out_shape=tuple(shapes),
        scratch_shapes=[
            pltpu.VMEM((steps, docs, features // steps), BF16),
            pltpu.VMEM(sketch.shape, BF16),
            pltpu.VMEM(sketch.shape, BF16),
            pltpu.VMEM((docs, columns), F32),
            pltpu.VMEM((owners * rows, docs), BF16),
        ]
        + [pltpu.VMEM(shape.shape, BF16) for shape in shapes]
        + [
            pltpu.SemaphoreType.DMA((2 * steps,)),
            pltpu.SemaphoreType.DMA((2 + owners // group,)),
        ],
        compiler_params=params(58),
        cost_estimate=cost(9),
        name="project",
    )(power, index.reshape(owners, 1, rows), images, sketch)


def gather_kernel(index_ref, table_ref, out_ref):
    docs = table_ref.shape[0]
    group, _, rows = index_ref.shape
    lane = lax.broadcasted_iota(jnp.int32, (rows, LANES), 1).astype(F32)
    hots = []
    for g in range(group):
        index = jnp.broadcast_to(index_ref[g].astype(F32), (LANES, rows)).T
        hots.append(
            jnp.concatenate(
                [jnp.where(index == lane + float(k), 1.0, 0.0).astype(BF16) for k in range(0, docs, LANES)],
                axis=1,
            )
        )
    found = jnp.dot(jnp.concatenate(hots, axis=0), table_ref[...], preferred_element_type=F32)
    out_ref[...] = found.astype(BF16).reshape(out_ref.shape)


def gather_rows(index, table):
    senders, rows = index.shape
    docs, columns = table.shape
    group = 4
    return pl.pallas_call(
        gather_kernel,
        grid=(senders // group,),
        in_specs=[
            pl.BlockSpec((group, 1, rows), lambda s: (s, 0, 0)),
            pl.BlockSpec((docs, columns), lambda s: (0, 0)),
        ],
        out_specs=pl.BlockSpec((group, rows, columns), lambda s: (s, 0, 0)),
        out_shape=jax.ShapeDtypeStruct((senders, rows, columns), BF16),
        compiler_params=params(58),
        cost_estimate=cost(3),
        name="gather_rows",
    )(index.reshape(senders, 1, rows), table)


def scale_kernel(block_ref, vals_ref, scale_ref, turned_ref, square_ref):
    square_ref[...] = jnp.zeros_like(square_ref)

    def slot(s, carry):
        weights = vals_ref[s].astype(F32)
        block = block_ref[s]
        square_ref[pl.ds(block, 1), :] += jnp.sum(weights * weights, axis=0, keepdims=True)
        turned_ref[s] = vals_ref[s].T
        return carry

    lax.fori_loop(0, vals_ref.shape[0], slot, 0)
    width = vals_ref.shape[2]
    for b in range(square_ref.shape[0]):
        root = lax.rsqrt(square_ref[b : b + 1, :] + 1.0)
        scale_ref[b * width : (b + 1) * width, :] = jnp.broadcast_to(root, (LANES, width)).T


def row_scales(blocks, vals):
    width = vals.shape[2]
    count = VOCAB_DEV // width
    return pl.pallas_call(
        scale_kernel,
        in_specs=[IN_SMEM, FULL_VMEM],
        out_specs=(FULL_VMEM, FULL_VMEM),
        out_shape=(
            jax.ShapeDtypeStruct((VOCAB_DEV, LANES), F32),
            jax.ShapeDtypeStruct((vals.shape[0], width, vals.shape[1]), BF16),
        ),
        scratch_shapes=[pltpu.VMEM((count, width), F32)],
        compiler_params=params(58),
        cost_estimate=cost(3),
        name="row_scales",
    )(blocks, vals)


def add_products(total_ref, vals_ref, rows_ref, block_ref, first_val, first_block, unroll):
    width = vals_ref.shape[1]

    def group(g, carry):
        parts = [
            jnp.dot(
                vals_ref[first_val + g * unroll + u],
                rows_ref[g * unroll + u],
                preferred_element_type=F32,
            )
            for u in range(unroll)
        ]
        for u in range(unroll):
            at = pl.multiple_of(block_ref[first_block + g * unroll + u] * width, width)
            total_ref[pl.ds(at, width), :] += parts[u]
        return carry

    lax.fori_loop(0, rows_ref.shape[0] // unroll, group, 0)


def begin_kernel(half_ref, block_ref, vals_ref, rows_ref, total_ref):
    total_ref[...] = jnp.zeros_like(total_ref)
    first = half_ref[0] * rows_ref.shape[0]
    add_products(total_ref, vals_ref, rows_ref, block_ref, first, first, 8)


def begin(half, blocks, vals, rows):
    return pl.pallas_call(
        begin_kernel,
        in_specs=[IN_SMEM] * 2 + [FULL_VMEM] * 2,
        out_specs=FULL_VMEM,
        out_shape=jax.ShapeDtypeStruct((VOCAB_DEV, rows.shape[2]), F32),
        compiler_params=params(58),
        cost_estimate=cost(5),
        name="begin",
    )(half, blocks, vals, rows)


def collect_kernel(earlier, started, half_ref, block_ref, vals_hbm, rows_hbm, scale_hbm, *refs):
    count = 2 * earlier
    if started:
        begun_hbm, refs = refs[0], refs[1:]
    before_hbm, refs = refs[:count], refs[count:]
    high_ref, low_ref, gram_ref, sum_ref, whole_ref, vals_ref, rows_ref, scale_ref = refs[:8]
    before, arrivals = refs[8 : 8 + count], refs[8 + count]
    begun_ref = refs[9 + count] if started else None
    part, _, columns = rows_ref.shape
    first = (1 - half_ref[0]) * part if started else 0
    moves = [(vals_hbm.at[pl.ds(first, part)], vals_ref), (rows_hbm, rows_ref), (scale_hbm, scale_ref)]
    if started:
        moves.append((begun_hbm, begun_ref))
    moves += list(zip(before_hbm, before))
    copies = [pltpu.make_async_copy(src, dst, arrivals.at[i]) for i, (src, dst) in enumerate(moves)]
    for copy in copies:
        copy.start()
    sum_ref[...] = jnp.zeros_like(sum_ref)
    for copy in copies[:2]:
        copy.wait()
    add_products(sum_ref, vals_ref, rows_ref, block_ref, 0, first, 8)
    for copy in copies[2:]:
        copy.wait()
    whole_ref[...] = jnp.zeros_like(whole_ref)
    step = 512

    def tile(t, carry):
        at = pl.ds(pl.multiple_of(t * step, step), step)
        scale = scale_ref[at, :]
        whole = sum_ref[at, :]
        if started:
            whole = whole + begun_ref[at, :]
        whole = whole * jnp.concatenate([scale] * (columns // LANES), axis=1)
        high, low = split2(whole)
        high_ref[at, :] = high
        low_ref[at, :] = low
        place = 0
        for e in range(earlier + 1):
            if e < earlier:
                other_high, other_low = before[2 * e][at, :], before[2 * e + 1][at, :]
            else:
                other_high, other_low = high, low
            wide = other_high.shape[1]
            whole_ref[:, place : place + wide] += (
                dot(high, other_high, 0, 0) + dot(low, other_high, 0, 0) + dot(high, other_low, 0, 0)
            )
            place += wide
        return carry

    lax.fori_loop(0, VOCAB_DEV // step, tile, 0)
    known = (whole_ref.shape[1] - columns) // LANES
    k = 0
    for r in range(columns // LANES):
        for c in range(known + r + 1):
            gram_ref[k] = whole_ref[r * LANES : (r + 1) * LANES, c * LANES : (c + 1) * LANES]
            k += 1


def collect(half, blocks, vals, scales, rows, begun, before):
    columns = rows.shape[2]
    known = sum(high.shape[1] for high, low in before)
    flat = [piece for pair in before for piece in pair]
    extra = [] if begun is None else [begun]
    rounds = columns // LANES
    count = sum(known // LANES + r + 1 for r in range(rounds))
    part = rows.shape[0]
    return pl.pallas_call(
        lambda *refs: collect_kernel(len(before), begun is not None, *refs),
        in_specs=[IN_SMEM] * 2 + [IN_HBM] * (3 + len(extra) + len(flat)),
        out_specs=(FULL_VMEM,) * 3,
        out_shape=(
            jax.ShapeDtypeStruct((VOCAB_DEV, columns), BF16),
            jax.ShapeDtypeStruct((VOCAB_DEV, columns), BF16),
            jax.ShapeDtypeStruct((count, LANES, LANES), F32),
        ),
        scratch_shapes=[
            pltpu.VMEM((VOCAB_DEV, columns), F32),
            pltpu.VMEM((columns, known + columns), F32),
            pltpu.VMEM((part,) + vals.shape[1:], BF16),
            pltpu.VMEM(rows.shape, BF16),
            pltpu.VMEM(scales.shape, F32),
        ]
        + [pltpu.VMEM(piece.shape, BF16) for piece in flat]
        + [pltpu.SemaphoreType.DMA((3 + len(extra) + len(flat),))]
        + [pltpu.VMEM(piece.shape, F32) for piece in extra],
        compiler_params=params(58),
        cost_estimate=cost(5),
        name="collect",
    )(half, blocks, vals, rows, scales, *extra, *flat)


def factor_block(rest_ref, unit_ref, upper_ref, inverse_ref):
    size = rest_ref.shape[0]
    lane = lax.broadcasted_iota(jnp.int32, (8, size), 1)
    sub = lax.broadcasted_iota(jnp.int32, (8, size), 0)

    def spread(row):
        return jnp.broadcast_to(row, (8, size))

    def pick(rows, wanted):
        return spread(jnp.sum(jnp.where(wanted, rows, 0.0), axis=1, keepdims=True))

    def panel(p, carry):
        rows, inverse, left, right = carry[:4]
        columns = list(carry[4:])
        first = pl.multiple_of(p * 8, 8)
        update = jnp.dot(left, right, preferred_element_type=F32)
        rest_ref[...] -= update[:, :size]
        unit_ref[...] -= update[:, size:]
        for j in range(8):
            root = lax.rsqrt(spread(columns[j][j : j + 1, :]))
            lower = columns[j] * root
            for m in range(j + 1, 8):
                columns[m] = columns[m] - lower * spread(lower[m : m + 1, :])
            below = jnp.where(sub > j, lower, 0.0)
            row = spread(rows[j : j + 1, :]) * root
            rows = jnp.where(sub == j, row, rows - below * row)
            row = spread(inverse[j : j + 1, :]) * root
            inverse = jnp.where(sub == j, row, inverse - below * row)
        rows = jnp.where(lane >= first + sub, rows, 0.0)
        upper_ref[pl.ds(first, 8), :] = rows
        inverse_ref[pl.ds(first, 8), :] = inverse
        after = pl.multiple_of(jnp.minimum(first + 8, size - 8), 8)
        next_rows = rest_ref[pl.ds(after, 8), :]
        next_inverse = unit_ref[pl.ds(after, 8), :]
        next_columns = [pick(next_rows, lane == after + j) for j in range(8)]
        spots = [pick(spread(rows[i : i + 1, :]), lane == after + sub) for i in range(8)]
        for i in range(8):
            for j in range(8):
                next_columns[j] = next_columns[j] - spots[i] * spread(spots[i][j : j + 1, :])
            next_rows = next_rows - spots[i] * spread(rows[i : i + 1, :])
            next_inverse = next_inverse - spots[i] * spread(inverse[i : i + 1, :])
        a, b, c = split3(rows)
        x, y, z = split3(inverse)
        left = jnp.concatenate([a, a, b, a, c, b], axis=0).T.astype(BF16)
        right = jnp.concatenate(
            [jnp.concatenate([a, b, a, c, a, b], axis=0), jnp.concatenate([x, y, x, z, x, y], axis=0)],
            axis=1,
        ).astype(BF16)
        return (next_rows, next_inverse, left, right, *next_columns)

    rows = rest_ref[:8, :]
    start = (
        rows,
        unit_ref[:8, :],
        jnp.zeros((size, 48), BF16),
        jnp.zeros((48, 2 * size), BF16),
        *[pick(rows, lane == j) for j in range(8)],
    )
    lax.fori_loop(0, size // 8, panel, start)


def gram_block(index, odd_ref, mine_ref, other_ref):
    half = mine_ref.shape[0]
    keep = odd_ref[0] == index // half
    return jnp.where(keep, mine_ref[index % half], other_ref[index % half])


def factor_row(first, count, odd_ref, mine_ref, other_ref, known_ref, work):
    rest_ref, unit_ref, piece_ref, small_ref = work
    square = (LANES, LANES)
    corner = gram_block(first + count, odd_ref, mine_ref, other_ref)
    left = None
    if count:
        row = [gram_block(first + k, odd_ref, mine_ref, other_ref) for k in range(count)]
        left = exact(jnp.concatenate(row, axis=1), known_ref[...], 1, 1)
        corner = corner - exact(left, left, 1, 1)
    rest_ref[...] = corner
    unit_ref[...] = jnp.where(
        lax.broadcasted_iota(jnp.int32, square, 0) == lax.broadcasted_iota(jnp.int32, square, 1), 1.0, 0.0
    )
    factor_block(rest_ref, unit_ref, piece_ref, small_ref)
    small = small_ref[...]
    inverse_row = -exact(small, exact(left, known_ref[...], 1, 0), 1, 0) if count else None
    return left, small, inverse_row


def cholesky_kernel(first, count, root, odd_ref, mine_ref, other_ref, *refs):
    known_ref = refs[0] if count else None
    inverse_ref, upper_ref = refs[-6:-4]
    work = refs[-4:]
    known = count * LANES
    left, small, inverse_row = factor_row(first, count, odd_ref, mine_ref, other_ref, known_ref, work)
    if count:
        inverse_ref[:known, :known] = known_ref[...]
        inverse_ref[:known, known:] = jnp.zeros((known, LANES), F32)
        inverse_ref[known:, :known] = inverse_row
        upper_ref[:known, :] = left.T * (1.0 / root)
    inverse_ref[known:, known:] = small
    upper_ref[known:, :] = work[2][...] * (1.0 / root)


def cholesky_step(odd, halves, first, count, inverse, root):
    total = (count + 1) * LANES
    inputs = [odd, *halves] + ([inverse] if count else [])
    square = pltpu.VMEM((LANES, LANES), F32)
    return pl.pallas_call(
        lambda *refs: cholesky_kernel(first, count, root, *refs),
        in_specs=[IN_SMEM] + [FULL_VMEM] * (len(inputs) - 1),
        out_specs=(FULL_VMEM,) * 2,
        out_shape=(
            jax.ShapeDtypeStruct((total, total), F32),
            jax.ShapeDtypeStruct((total, LANES), F32),
        ),
        scratch_shapes=[square] * 4,
        compiler_params=params(16),
        cost_estimate=cost(8),
        name="cholesky_step",
    )(*inputs)


def finish_kernel(first, count, pieces, root, odd_ref, mine_ref, other_ref, known_ref, *refs):
    before, refs = refs[:count], refs[count:]
    pieces_hbm, refs = refs[: 2 * pieces], refs[2 * pieces + 1 :]
    basis_hbm, upper_ref = refs[:2]
    work = refs[2:6]
    stage_ref, arrivals, departures = refs[6:9]
    held = refs[9:]
    known = count * LANES
    copies = [
        pltpu.make_async_copy(src, dst, arrivals.at[i]) for i, (src, dst) in enumerate(zip(pieces_hbm, held))
    ]
    for copy in copies:
        copy.start()
    left, small, inverse_row = factor_row(first, count, odd_ref, mine_ref, other_ref, known_ref, work)
    row_high, row_low = split2(jnp.concatenate([inverse_row, small], axis=1))
    for copy in copies:
        copy.wait()
    steps, step = stage_ref.shape[:2]
    sent = []
    for t in range(steps):
        at = slice(t * step, (t + 1) * step)
        total = None
        place = 0
        for e in range(pieces):
            high, low = held[2 * e][at, :], held[2 * e + 1][at, :]
            wide = high.shape[1]
            high_part, low_part = row_high[:, place : place + wide], row_low[:, place : place + wide]
            term = dot(high, high_part, 1, 1) + dot(low, high_part, 1, 1) + dot(high, low_part, 1, 1)
            total = term if total is None else total + term
            place += wide
        stage_ref[t] = total * root
        copy = pltpu.make_async_copy(
            stage_ref.at[t], basis_hbm.at[pl.ds(t * step, step), pl.ds(known, LANES)], departures.at[t]
        )
        copy.start()
        sent.append(copy)
    upper_ref[...] = jnp.zeros_like(upper_ref)
    for e in range(count):
        upper_ref[: (e + 1) * LANES, e * LANES : (e + 1) * LANES] = before[e][...]
    upper_ref[:known, known:] = left.T * (1.0 / root)
    upper_ref[known:, known:] = work[2][...] * (1.0 / root)
    for copy in sent:
        copy.wait()


def finish(odd, halves, first, inverse, before, pieces, basis, root):
    count = len(before)
    total = (count + 1) * LANES
    flat = [piece for pair in pieces for piece in pair]
    inputs = [odd, *halves, inverse, *before, *flat, basis]
    steps = 4
    square = pltpu.VMEM((LANES, LANES), F32)
    return pl.pallas_call(
        lambda *refs: finish_kernel(first, count, len(pieces), root, *refs),
        in_specs=[IN_SMEM] + [FULL_VMEM] * (3 + count) + [IN_HBM] * (len(flat) + 1),
        out_specs=(IN_HBM, FULL_VMEM),
        out_shape=(
            jax.ShapeDtypeStruct(basis.shape, F32),
            jax.ShapeDtypeStruct((total, total), F32),
        ),
        scratch_shapes=[square] * 4
        + [
            pltpu.VMEM((steps, VOCAB_DEV // steps, LANES), F32),
            pltpu.SemaphoreType.DMA((len(flat),)),
            pltpu.SemaphoreType.DMA((steps,)),
        ]
        + [pltpu.VMEM(piece.shape, BF16) for piece in flat],
        input_output_aliases={len(inputs) - 1: 0},
        compiler_params=params(58),
        cost_estimate=cost(12),
        name="finish",
    )(*inputs)


def basis_kernel(pieces, known, root, inverse_ref, *refs):
    out_ref = refs[-1]
    total = None
    place = 0
    for e in range(pieces):
        high, low = refs[2 * e][...], refs[2 * e + 1][...]
        wide = high.shape[1]
        part_high, part_low = split2(inverse_ref[known:, place : place + wide])
        term = dot(high, part_high, 1, 1) + dot(low, part_high, 1, 1) + dot(high, part_low, 1, 1)
        total = term if total is None else total + term
        place += wide
    out_ref[...] = total * root


def basis_block(inverse, pieces, buffer, root, columns_total):
    columns = pieces[-1][0].shape[1]
    total = inverse.shape[0]
    known = total - columns
    step = 512
    flat = [piece for pair in pieces for piece in pair]
    in_specs = [pl.BlockSpec((total, total), lambda t: (0, 0))]
    in_specs += [pl.BlockSpec((step, piece.shape[1]), lambda t: (t, 0)) for piece in flat]
    inputs = [inverse] + flat
    aliases = {}
    if buffer is not None:
        aliases = {len(inputs): 0}
        inputs.append(buffer)
        in_specs.append(pl.BlockSpec(memory_space=pl.ANY))
    return pl.pallas_call(
        lambda *refs: basis_kernel(len(pieces), known, root, *refs),
        grid=(VOCAB_DEV // step,),
        in_specs=in_specs,
        out_specs=pl.BlockSpec((step, columns), lambda t: (t, known // columns)),
        out_shape=jax.ShapeDtypeStruct((VOCAB_DEV, columns_total), F32),
        input_output_aliases=aliases,
        compiler_params=params(58),
        cost_estimate=cost(3),
        name="basis_block",
    )(*inputs)


def swap(x, axis, bit):
    size = lax.axis_size(axis)
    return lax.ppermute(x, axis, [(i, i ^ bit) for i in range(size)])


def bits(axis):
    size = lax.axis_size(axis)
    return [1 << k for k in range(size.bit_length() - 1)]


def sum_all(x):
    for axis in ("half", "rest", "docs"):
        for bit in reversed(bits(axis)):
            x = x + swap(x, axis, bit)
    return x


def sum_halves(x):
    half = x.shape[0] // 2
    odd = lax.axis_index("docs") % 2
    mine = lax.dynamic_slice_in_dim(x, odd * half, half)
    other = lax.dynamic_slice_in_dim(x, (1 - odd) * half, half)
    mine = mine + swap(other, "docs", 1)
    for axis in ("docs", "rest", "half"):
        for bit in bits(axis):
            if axis != "docs" or bit > 1:
                mine = mine + swap(mine, axis, bit)
    other = swap(mine, "docs", 1)
    return mine, other


def body(images, sketch, tile_vals, tile_rows, tile_count, tile_block):
    side = lax.axis_size("rest") * lax.axis_size("docs")
    senders = 2 * side
    doc_rows = images.shape[0]
    capacity, tile_height, tile_width = tile_vals.shape[2:]
    columns = sketch.shape[1]
    slots = senders * capacity
    cut = FIRST_PART * LANES
    half = lax.axis_index("half")
    outgoing, power = prepare(tile_count, images, tile_vals)
    vals = lax.all_to_all(
        outgoing.reshape(senders, capacity * tile_height, tile_width), BOTH, 0, 0, tiled=True
    )
    vals = vals.reshape(slots, tile_height, tile_width)
    power = sum_all(power)
    index = tile_rows[0].reshape(senders, capacity * tile_height)
    halves = index.reshape(2, side, capacity * tile_height)
    near_index = lax.dynamic_index_in_dim(halves, half, 0, keepdims=False)
    far_index = swap(lax.dynamic_index_in_dim(halves, 1 - half, 0, keepdims=False), "half", 1)
    blocks = tile_block[0].reshape(slots)
    root = math.sqrt(VOCAB_DEV * senders)
    scale, turned = row_scales(blocks, vals)
    where = half.reshape(1).astype(jnp.int32)
    table, last_table, near = project(power, near_index, images, sketch, doc_rows * senders, cut)
    far_table = swap(table, "half", 1)
    near = lax.all_to_all(near, SIDE, 0, 0, tiled=True)
    far = gather_rows(far_index, far_table)
    far = lax.all_to_all(far, SIDE, 0, 0, tiled=True)
    final = gather_rows(index, last_table)
    final = lax.all_to_all(final, BOTH, 0, 0, tiled=True)

    def by_slot(rows):
        return rows.reshape(-1, tile_height, rows.shape[2])

    odd = (lax.axis_index("docs") % 2).reshape(1).astype(jnp.int32)
    begun = begin(where, blocks, turned, by_slot(near))
    pieces, uppers = [], []
    inverse = basis = None
    for c, rows in enumerate([by_slot(far), by_slot(final)]):
        high, low, gram = collect(where, blocks, turned, scale, rows, begun if c == 0 else None, pieces)
        pieces.append((high, low))
        grams = sum_halves(gram)
        first = 0
        for _ in range(high.shape[1] // LANES):
            count = len(uppers)
            if (count + 1) * LANES == columns:
                return finish(odd, grams, first, inverse, uppers, pieces, basis, root)
            inverse, upper = cholesky_step(odd, grams, first, count, inverse, root)
            uppers.append(upper)
            first += count + 1
        basis = basis_block(inverse, pieces, basis, root, columns)


def solution(mesh):
    split = (2, mesh.shape["vocab"] // 2, mesh.shape["docs"])
    finer = jax.sharding.Mesh(mesh.devices.reshape(split), BOTH)
    placed = (
        P(BOTH, None),
        P(),
        P(BOTH, None, None, None, None),
        P(BOTH, None, None, None),
        P(BOTH, None),
        P(BOTH, None, None),
    )
    return jax.shard_map(
        body,
        mesh=finer,
        in_specs=placed,
        out_specs=(P(BOTH, None), P()),
        check_vma=False,
    )
```
